32 devices in a mesh: grp: 2 (over core), tile: 16 (over z, y, x).
Axes of the slice: x: 2, y: 2, z: 4, core: 2. Of those that a mesh axis runs over, the one named last changes fastest.
Arguments:
- attn_input: bfloat16 [2048, 4096], P(('grp', 'tile')), may hold values from -9 to 9
- mlp_input: bfloat16 [2048, 4096], P(('grp', 'tile')), may hold values from -9 to 9
Outputs:
- hess_attn: float32 [16, 1024, 1024], P('tile', 'grp')
- hess_mlp: float32 [16, 1024, 1024], P('tile', 'grp')
The draws below stay inside these ranges and needn't reach their ends.
All inputs are finite; a program needn't handle non-finite values.
Results may differ from the reference program's by a relative error of at most 0.0003.
Values may be sent and summed in bfloat16 or wider, within the bound.
No kernel may reach another device: no remote copies, remote signals or barrier semaphores. Data moves between devices by JAX's collectives and lax.ppermute only.
A program may use at most 192 MiB of HBM per device.

```python
import jax
import jax.numpy as jnp
from jax import lax

W = 4096
ROWB = 4
TOKENS = 2048
COLB = 4
RT = 1024
CT = 1024


def block_levels(rng, dims, pieces, least, largest):
    level = 1.0
    for axis_at, shards_of in pieces:
        draws = jax.random.uniform(jax.random.fold_in(jax.random.fold_in(rng, 6), axis_at), (shards_of,), jnp.float32, least / len(pieces), largest / len(pieces))
        level = level * jnp.repeat(jnp.exp(draws), dims[axis_at] // shards_of).reshape((-1,) + (1,) * (len(dims) - 1 - axis_at))
    return level


def gaussian(key, dims, width, reach, cuts=(), dtype=jnp.bfloat16):
    array = jax.random.normal(key, dims, jnp.float32) * width
    if len(cuts) > 0:
        array = block_levels(key, dims, cuts, -0.22, 0.18) * array
    return jnp.clip(array, min=-reach, max=reach).astype(dtype)


def setup_inputs(seed: int = 0) -> dict:
    key_of = jax.random.split(jax.random.key(seed), 3)
    return {
        "attn_input": gaussian(key_of[0], (TOKENS, W), 1.5, 9.0, ((0, 32),)),
        "mlp_input": gaussian(key_of[1], (TOKENS, W), 1.5, 9.0, ((0, 32),)),
    }


def hessian_tiles(inputs):
    widened = inputs.astype(jnp.float32)
    gram_full = jnp.dot(widened.T, widened, precision=lax.Precision.HIGHEST)
    gram_full = gram_full * (2.0 / TOKENS)
    tiled = gram_full.reshape(ROWB, RT, COLB, CT).transpose(0, 2, 1, 3)
    return tiled.reshape(ROWB * COLB, RT, CT)


def reference(attn_input, mlp_input):
    return (hessian_tiles(attn_input), hessian_tiles(mlp_input))
```

```python
import jax
import jax.numpy as jnp
from jax import lax
from jax.sharding import PartitionSpec as P

ROWB = 4


def xor_rows(k, cols):
    return [(r * cols + c, (r ^ k) * cols + c) for r in range(ROWB) for c in range(cols)]


def xor_cols(k, cols):
    return [(r * cols + c, r * cols + (c ^ k)) for r in range(ROWB) for c in range(cols)]


def forward_rows(cols):
    return [(r * cols + c, d * cols + c) for r, d in ((0, 2), (3, 1), (2, 3), (1, 0)) for c in range(cols)]


def block(x, index, width):
    return lax.dynamic_slice_in_dim(x, index * width, width, 1)


def send(x, perm):
    return lax.ppermute(x, "tile", perm)


def gather(x, cols):
    tok, feat = x.shape
    me = lax.axis_index("tile")
    r, c = me // cols, me % cols
    rw, cw = feat // ROWB, feat // cols
    order = (0, 1, 3, 2)
    own_rows = [block(x, r, rw)] + [send(block(x, r ^ q, rw), xor_rows(q, cols)) for q in order[1:]]
    own_cols = [block(x, c, cw)] + [send(block(x, c ^ k, cw), xor_cols(k, cols)) for k in range(1, cols)]
    y = jnp.concatenate(own_cols, 0)
    p3 = send(y, xor_rows(3, cols))
    p1 = send(y, xor_rows(1, cols))
    rows = jnp.concatenate(own_rows, 0)
    all_rows = [rows] + [send(rows, xor_cols(k, cols)) for k in range(1, cols)]
    outer = (r == 0) | (r == ROWB - 1)
    p2 = send(jnp.where(outer, y, p3), forward_rows(cols))
    row_pieces = [jnp.concatenate([a[i * tok:(i + 1) * tok] for a in all_rows], 0) for i in range(ROWB)]
    return row_pieces, [y, p1, p3, p2]


def dot(a, b):
    return lax.dot_general(a, b, (((0,), (0,)), ((), ())), preferred_element_type=jnp.float32)


def hessian(x, tiles, groups):
    cols = tiles // ROWB
    row_pieces, col_pieces = gather(x, cols)
    head_r, head_c = jnp.concatenate(row_pieces[:-1], 0), jnp.concatenate(col_pieces[:-1], 0)
    tail_r, tail_c = row_pieces[-1], col_pieces[-1]
    factor = 2.0 / (x.shape[0] * tiles * groups)
    if groups == 2:
        g = lax.axis_index("grp")
        half = head_r.shape[1] // groups
        part = lambda i: dot(block(head_r, i, half), head_c) + dot(block(tail_r, i, half), tail_c)
        theirs = lax.ppermute(part(1 - g), "grp", [(0, 1), (1, 0)])
        share = part(g) + theirs
    else:
        share = lax.psum_scatter(dot(head_r, head_c) + dot(tail_r, tail_c), "grp", scatter_dimension=0, tiled=True)
    return (share * factor)[None]


def solution(mesh):
    tiles, groups = mesh.shape["tile"], mesh.shape["grp"]

    def body(attn_input, mlp_input):
        return hessian(attn_input, tiles, groups), hessian(mlp_input, tiles, groups)

    in_specs = (P(("grp", "tile"), None), P(("grp", "tile"), None))
    out_specs = (P("tile", "grp", None), P("tile", "grp", None))
    return jax.shard_map(body, mesh=mesh, in_specs=in_specs, out_specs=out_specs, check_vma=False)
```

```python
import jax
import jax.numpy as jnp
from jax import lax
from jax.sharding import PartitionSpec as P

ROWB = 4


def xor_rows(k, cols):
    return [(r * cols + c, (r ^ k) * cols + c) for r in range(ROWB) for c in range(cols)]


def xor_cols(k, cols):
    return [(r * cols + c, r * cols + (c ^ k)) for r in range(ROWB) for c in range(cols)]


def forward_rows(cols):
    return [(r * cols + c, d * cols + c) for r, d in ((0, 2), (3, 1), (2, 3), (1, 0)) for c in range(cols)]


def block(x, index, width):
    return lax.dynamic_slice_in_dim(x, index * width, width, 1)


def send(x, perm):
    return lax.ppermute(x, "tile", perm)


def sibling(x):
    return lax.ppermute(x, "grp", [(0, 1), (1, 0)])


def dot(a, b):
    return lax.dot_general(a, b, (((0,), (0,)), ((), ())), preferred_element_type=jnp.float32)


def where_am_i(cols):
    me = lax.axis_index("tile")
    return me // cols, me % cols


def gather_then_split(x, cols):
    r, c = where_am_i(cols)
    rw, cw = x.shape[1] // ROWB, x.shape[1] // cols
    outer = (r == 0) | (r == ROWB - 1)
    p3 = send(x, xor_rows(3, cols))
    p1 = send(x, xor_rows(1, cols))
    p2 = send(jnp.where(outer, x, p3), forward_rows(cols))
    got = []
    for piece in (x, jnp.concatenate([p1, p3], 0), p2):
        mine = block(piece, r, rw)
        got.append(jnp.concatenate([mine, block(piece, c, cw)], 1))
        for k in range(1, cols):
            got.append(send(jnp.concatenate([mine, block(piece, c ^ k, cw)], 1), xor_cols(k, cols)))
    got = jnp.concatenate(got, 0)
    return got[:, :rw], got[:, rw:]


def split_then_gather(x, cols):
    tok, feat = x.shape
    r, c = where_am_i(cols)
    rw, cw = feat // ROWB, feat // cols
    order = (0, 1, 3, 2)
    own_rows = [block(x, r, rw)] + [send(block(x, r ^ q, rw), xor_rows(q, cols)) for q in order[1:]]
    own_cols = [block(x, c, cw)] + [send(block(x, c ^ k, cw), xor_cols(k, cols)) for k in range(1, cols)]
    y = jnp.concatenate(own_cols, 0)
    p3 = send(y, xor_rows(3, cols))
    p1 = send(y, xor_rows(1, cols))
    rows = jnp.concatenate(own_rows, 0)
    all_rows = [rows] + [send(rows, xor_cols(k, cols)) for k in range(1, cols)]
    outer = (r == 0) | (r == ROWB - 1)
    row_pieces = [jnp.concatenate([a[i * tok:(i + 1) * tok] for a in all_rows], 0) for i in range(ROWB)]
    return row_pieces, [y, p1, p3], jnp.where(outer, y, p3)


def share_of(rows, columns):
    groups = lax.axis_size("grp")
    if groups != 2:
        return lax.psum_scatter(dot(rows, columns), "grp", scatter_dimension=0, tiled=True)
    g = lax.axis_index("grp")
    half = rows.shape[1] // groups
    theirs = sibling(dot(block(rows, 1 - g, half), columns))
    return dot(block(rows, g, half), columns) + theirs


def solution(mesh):
    tiles, groups = mesh.shape["tile"], mesh.shape["grp"]
    cols = tiles // ROWB

    def body(attn_input, mlp_input):
        factor = 2.0 / (attn_input.shape[0] * tiles * groups)
        attn = share_of(*gather_then_split(attn_input, cols)) * factor
        row_pieces, col_pieces, last = split_then_gather(mlp_input, cols)
        attn, last = lax.optimization_barrier((attn, last))
        last_cols = send(last, forward_rows(cols))
        mlp = share_of(jnp.concatenate(row_pieces[:-1], 0), jnp.concatenate(col_pieces, 0))
        if groups == 2:
            g = lax.axis_index("grp")
            half = mlp.shape[0]
            their_rows = sibling(block(row_pieces[-1], 1 - g, half))
            their_cols = sibling(last_cols)
            mlp = mlp + dot(block(row_pieces[-1], g, half), last_cols) + dot(their_rows, their_cols)
        else:
            mlp = mlp + share_of(row_pieces[-1], last_cols)
        return attn[None], (mlp * factor)[None]

    in_specs = (P(("grp", "tile"), None), P(("grp", "tile"), None))
    out_specs = (P("tile", "grp", None), P("tile", "grp", None))
    return jax.shard_map(body, mesh=mesh, in_specs=in_specs, out_specs=out_specs, check_vma=False)
```

```python
import jax
import jax.numpy as jnp
from jax import lax
from jax.sharding import PartitionSpec as P

ROWB = 4


def xor_rows(k, cols):
    return [(r * cols + c, (r ^ k) * cols + c) for r in range(ROWB) for c in range(cols)]


def xor_cols(k, cols):
    return [(r * cols + c, r * cols + (c ^ k)) for r in range(ROWB) for c in range(cols)]


def forward_rows(cols):
    return [(r * cols + c, d * cols + c) for r, d in ((0, 2), (3, 1), (2, 3), (1, 0)) for c in range(cols)]


def block(x, index, width):
    return lax.dynamic_slice_in_dim(x, index * width, width, 1)


def send(x, perm):
    return lax.ppermute(x, "tile", perm)


def sibling(x):
    return lax.ppermute(x, "grp", [(0, 1), (1, 0)])


def dot(a, b):
    return lax.dot_general(a, b, (((0,), (0,)), ((), ())), preferred_element_type=jnp.float32)


def where_am_i(cols):
    me = lax.axis_index("tile")
    return me // cols, me % cols


def halves(x, k, cols):
    r, c = where_am_i(cols)
    rw, cw = x.shape[1] // ROWB, x.shape[1] // cols
    return jnp.concatenate([block(x, r, rw), block(x, c ^ k, cw)], 1)


def split(x, cols):
    got = [halves(x, 0, cols)] + [send(halves(x, k, cols), xor_cols(k, cols)) for k in range(1, cols)]
    got = jnp.concatenate(got, 0)
    rw = x.shape[1] // ROWB
    return got[:, :rw], got[:, rw:]


def finish(head, tail, factor):
    groups = lax.axis_size("grp")
    if groups != 2:
        total = sum(dot(a, b) for a, b in head + [tail])
        return lax.psum_scatter(total, "grp", scatter_dimension=0, tiled=True) * factor
    g = lax.axis_index("grp")
    half = tail[0].shape[1] // groups
    theirs = sibling(sum(dot(block(a, 1 - g, half), b) for a, b in head))
    share = sum(dot(block(a, g, half), b) for a, b in head) + theirs
    their_rows = sibling(block(tail[0], 1 - g, half))
    their_cols = sibling(tail[1])
    share = share + dot(block(tail[0], g, half), tail[1]) + dot(their_rows, their_cols)
    return share * factor


def solution(mesh):
    tiles, groups = mesh.shape["tile"], mesh.shape["grp"]
    cols = tiles // ROWB

    def body(attn_input, mlp_input):
        tok, feat = attn_input.shape
        r, c = where_am_i(cols)
        rw, cw = feat // ROWB, feat // cols
        outer = (r == 0) | (r == ROWB - 1)
        factor = 2.0 / (tok * tiles * groups)

        a, m = attn_input, mlp_input
        a3, a1 = send(a, xor_rows(3, cols)), send(a, xor_rows(1, cols))
        m_cols = [block(m, c, cw)] + [send(block(m, c ^ k, cw), xor_cols(k, cols)) for k in range(1, cols)]
        own_rows = [block(m, r, rw)] + [send(block(m, r ^ q, rw), xor_rows(q, cols)) for q in (1, 3, 2)]
        y = jnp.concatenate(m_cols, 0)
        own = split(a, cols)
        a3, y = lax.optimization_barrier((a3, y))
        a2 = send(jnp.where(outer, a, a3), forward_rows(cols))
        m3, m1 = send(y, xor_rows(3, cols)), send(y, xor_rows(1, cols))
        rows = jnp.concatenate(own_rows, 0)
        all_rows = [rows] + [send(rows, xor_cols(k, cols)) for k in range(1, cols)]
        mid = split(jnp.concatenate([a1, a3], 0), cols)
        a2, m3 = lax.optimization_barrier((a2, m3))
        m2 = send(jnp.where(outer, y, m3), forward_rows(cols))
        last = split(a2, cols)
        row_pieces = [jnp.concatenate([x[i * tok:(i + 1) * tok] for x in all_rows], 0) for i in range(ROWB)]
        col_pieces = [y, m1, m3, m2]
        attn = finish([own, mid], last, factor)
        m_head = (jnp.concatenate(row_pieces[:-1], 0), jnp.concatenate(col_pieces[:-1], 0))
        mlp = finish([m_head], (row_pieces[-1], col_pieces[-1]), factor)
        return attn[None], mlp[None]

    in_specs = (P(("grp", "tile"), None), P(("grp", "tile"), None))
    out_specs = (P("tile", "grp", None), P("tile", "grp", None))
    return jax.shard_map(body, mesh=mesh, in_specs=in_specs, out_specs=out_specs, check_vma=False)
```

```python
import jax
import jax.numpy as jnp
from jax import lax
from jax.sharding import PartitionSpec as P


ROWB = 4


def xor_rows(k, cols):
    return [(r * cols + c, (r ^ k) * cols + c) for r in range(ROWB) for c in range(cols)]


def xor_cols(k, cols):
    return [(r * cols + c, r * cols + (c ^ k)) for r in range(ROWB) for c in range(cols)]


def swap_rows(pairs, cols):
    return [(r * cols + c, d * cols + c) for r, d in pairs for c in range(cols)]


def forward_rows(cols):
    return [(r * cols + c, d * cols + c) for r, d in ((0, 2), (3, 1), (2, 3), (1, 0)) for c in range(cols)]


def block(x, index, width):
    return lax.dynamic_slice_in_dim(x, index * width, width, 1)


def send(x, perm):
    return lax.ppermute(x, "tile", perm)


def sibling(x):
    return lax.ppermute(x, "grp", [(0, 1), (1, 0)])


def dot(a, b):
    return lax.dot_general(a, b, (((0,), (0,)), ((), ())), preferred_element_type=jnp.float32)


def where_am_i(cols):
    me = lax.axis_index("tile")
    return me // cols, me % cols


def halves(x, k, cols):
    r, c = where_am_i(cols)
    rw, cw = x.shape[1] // ROWB, x.shape[1] // cols
    return jnp.concatenate([block(x, r, rw), block(x, c ^ k, cw)], 1)


def finish(head, tail, factor):
    groups = lax.axis_size("grp")
    if groups != 2:
        total = sum(dot(a, b) for a, b in head + [tail])
        return lax.psum_scatter(total, "grp", scatter_dimension=0, tiled=True) * factor
    g = lax.axis_index("grp")
    half = tail[0].shape[1] // groups
    theirs = sibling(sum(dot(block(a, 1 - g, half), b) for a, b in head))
    share = sum(dot(block(a, g, half), b) for a, b in head) + theirs
    their_rows = sibling(block(tail[0], 1 - g, half))
    their_cols = sibling(tail[1])
    share = share + dot(block(tail[0], g, half), tail[1]) + dot(their_rows, their_cols)
    return share * factor


def solution(mesh):
    tiles, groups = mesh.shape["tile"], mesh.shape["grp"]
    cols = tiles // ROWB

    def body(attn_input, mlp_input):
        tok, feat = attn_input.shape
        r, c = where_am_i(cols)
        rw, cw = feat // ROWB, feat // cols
        outer = (r == 0) | (r == ROWB - 1)
        factor = 2.0 / (tok * tiles * groups)

        a, m = attn_input, mlp_input

        def beside(k):
            return jnp.concatenate([a, block(m, r ^ k, rw)], 1)

        z3 = send(beside(3), xor_rows(3, cols))
        z1 = send(beside(1), xor_rows(1, cols))
        first = [jnp.concatenate([halves(a, 0, cols), block(m, c, cw)], 1)]
        for k in range(1, cols):
            first.append(send(jnp.concatenate([halves(a, k, cols), block(m, c ^ k, cw)], 1), xor_cols(k, cols)))
        r2 = send(block(m, r ^ 2, rw), xor_rows(2, cols))
        first = jnp.concatenate(first, 0)
        own, y = (first[:, :rw], first[:, rw:rw + cw]), first[:, rw + cw:]
        a3, a1 = z3[:, :feat], z1[:, :feat]
        z3, y = lax.optimization_barrier((z3, y))
        a3 = z3[:, :feat]
        a2 = send(jnp.where(outer, a, a3), forward_rows(cols))
        m3 = send(y, swap_rows(((1, 2), (2, 1)), cols))
        m1 = send(y, xor_rows(1, cols))
        lo = jnp.concatenate([block(m, r, rw), z1[:, feat:]], 0)
        hi = jnp.concatenate([z3[:, feat:], r2], 0)
        both = jnp.concatenate([a1, a3], 0)
        second = [jnp.concatenate([lo, hi, halves(both, 0, cols)], 1)]
        for k in range(1, cols):
            second.append(send(jnp.concatenate([lo, hi, halves(both, k, cols)], 1), xor_cols(k, cols)))
        a2, m3 = lax.optimization_barrier((a2, m3))
        m2 = send(jnp.where(outer, y, m3), forward_rows(cols))
        m3_far = send(y, swap_rows(((0, 3), (3, 0)), cols))
        last = [halves(a2, 0, cols)] + [send(halves(a2, k, cols), xor_cols(k, cols)) for k in range(1, cols)]
        last = jnp.concatenate(last, 0)
        second_all = jnp.concatenate(second, 0)
        mid = (second_all[:, 2 * rw:3 * rw], second_all[:, 3 * rw:])
        attn = finish([own, mid], (last[:, :rw], last[:, rw:]), factor)

        def rows_of(q):
            at, to = (q % 2) * tok, (q // 2) * rw
            return jnp.concatenate([x[at:at + tok, to:to + rw] for x in second], 0)

        m3 = jnp.where(outer, m3_far, m3)
        m_head = (jnp.concatenate([rows_of(0), rows_of(1)], 0), jnp.concatenate([y, m1], 0))
        m_tail = (jnp.concatenate([rows_of(2), rows_of(3)], 0), jnp.concatenate([m3, m2], 0))
        mlp = finish([m_head], m_tail, factor)
        return attn[None], mlp[None]

    in_specs = (P(("grp", "tile"), None), P(("grp", "tile"), None))
    out_specs = (P("tile", "grp", None), P("tile", "grp", None))
    return jax.shard_map(body, mesh=mesh, in_specs=in_specs, out_specs=out_specs, check_vma=False)
```
